128 devices in a mesh: row: 16 (over y, z), col: 8 (over x, core).
Axes of the slice: x: 4, y: 4, z: 4, core: 2. Of those that a mesh axis runs over, the one named last changes fastest.
Arguments:
- matrix: float32 [4096, 4096], P('row', 'col'), may hold values from -0.92 to 1.92, as said below
Outputs:
- inverse: float32 [4096, 4096], P('row', 'col')
- residual_norms: float32 [4], replicated
The draws below stay inside these ranges and needn't reach their ends.
Inputs may be any that keep to these rules, and one draw needn't show every extreme that they name: matrix is exactly symmetric and positive definite; all its eigenvalues lie between 0.08 and 1.92.
All inputs are finite; a program needn't handle non-finite values.
Results may differ from the reference program's by a relative error of at most 0.0017.
The reference program's roundings to bfloat16 on the way (of `mat_low`, `cur_low` and `shift_low`) count: a program that leaves them out, or rounds other values in their place, can miss the bound.
Values may be sent and summed in bfloat16 or wider, within the bound.
A program may use at most 64 MiB of HBM per device.

```python
import jax
import jax.numpy as jnp
from jax import lax

N = 4096
ITERS = 4


def draw_matrix(key, part):
    noise_key = jax.random.fold_in(key, 17)
    noise_draw = jnp.clip(jax.random.normal(noise_key, (N, N), jnp.float32), -4.0, 4.0)
    spread = 0.9
    wigner = (noise_draw + noise_draw.T) * (0.5 / (1.4142135 * jnp.sqrt(jnp.float32(N))))
    identity = jnp.eye(N, dtype=jnp.float32)
    for polish in range(3):
        square = jnp.dot(wigner, wigner, precision=lax.Precision.HIGHEST)
        wigner = jnp.dot(wigner, 1.5 * identity - 0.5 * square, precision=lax.Precision.HIGHEST)
    shaped = 0.5 * (wigner + wigner.T)
    return identity + spread * shaped


def setup_inputs(seed: int = 0) -> dict:
    key_list = jax.random.split(jax.random.key(seed), 2)
    return {
        "matrix": draw_matrix(jax.random.fold_in(key_list[1], 71), 0),
    }


def reference(matrix):
    mat_low = matrix.astype(jnp.bfloat16)
    sq_total = jnp.sum(matrix * matrix)
    start_scale = jnp.sqrt(jnp.float32(N)) / jnp.sqrt(sq_total)
    identity = jnp.eye(N, dtype=jnp.float32)
    current = start_scale * identity
    norm_list = []
    for iteration in range(ITERS):
        cur_low = current.astype(jnp.bfloat16)
        product = jnp.dot(mat_low, cur_low, preferred_element_type=jnp.float32)
        residual = identity - product
        norm_list.append(jnp.sqrt(jnp.sum(residual * residual) / N))
        shift_low = (identity + residual).astype(jnp.bfloat16)
        current = jnp.dot(cur_low, shift_low, preferred_element_type=jnp.float32)
    return (current, jnp.stack(norm_list))
```

```python
import functools

import jax
import jax.numpy as jnp
from jax import lax
from jax.sharding import Mesh
from jax.sharding import PartitionSpec as P

N = 4096
ITERS = 4
ROW = ("row_0", "row_1")
COL = ("col_0", "col_1")
ROW_COL = ("row_0", "row_1", "col_0", "col_1")


def over_axes(x, axes):
    return functools.reduce(lax.psum, axes, x)


def laid_out(pieces, dim):
    dims = list(pieces.shape[1:])
    dims[dim] *= pieces.shape[0]
    return jnp.moveaxis(pieces, 0, dim).reshape(dims)


def sent_to_all(x, axis):
    count = lax.axis_size(axis)
    return lax.all_to_all(jnp.broadcast_to(x[None], (count, *x.shape)), axis, 0, 0, tiled=True)


def collect(x, axis, dim):
    return laid_out(sent_to_all(x, axis), dim)


def eye_at(shape, row0, col0):
    rows = row0 + lax.broadcasted_iota(jnp.int32, shape, 0)
    cols = col0 + lax.broadcasted_iota(jnp.int32, shape, 1)
    return (rows == cols).astype(jnp.float32)


def shards(matrix):
    row_count, col_count = matrix.shape
    row0 = lax.axis_index(ROW) * row_count
    col0 = lax.axis_index(COL) * col_count
    sq_total = over_axes(jnp.sum(matrix * matrix), ROW_COL)
    start_scale = jnp.sqrt(jnp.float32(N)) / jnp.sqrt(sq_total)
    scale_low = start_scale.astype(jnp.bfloat16).astype(jnp.float32)
    eye_block = eye_at(matrix.shape, row0, col0)
    mat_low = matrix.astype(jnp.bfloat16)
    panel_rows = collect(mat_low, COL, 1)
    panel_cols = lax.all_gather(mat_low, ROW, axis=0, tiled=True)

    def first(mat, eye):
        residual = eye - scale_low * mat.astype(jnp.float32)
        shift_low = (eye + residual).astype(jnp.bfloat16)
        return residual, (scale_low * shift_low.astype(jnp.float32)).astype(jnp.bfloat16)

    residual, _ = first(mat_low, eye_block)
    partial_list = [jnp.sum(residual * residual)]
    _, iterate_rows = first(panel_rows, eye_at(panel_rows.shape, row0, 0))
    _, iterate_cols = first(panel_cols, eye_at(panel_cols.shape, 0, col0))
    for iteration in range(1, ITERS):
        if iteration > 1:
            cur_low = current.astype(jnp.bfloat16)
            iterate_cols = lax.all_gather(cur_low, ROW, axis=0, tiled=True)
            iterate_rows = collect(cur_low, COL, 1)
        product = jnp.dot(panel_rows, iterate_cols, preferred_element_type=jnp.float32)
        residual = eye_block - product
        partial_list.append(jnp.sum(residual * residual))
        shift_low = (eye_block + residual).astype(jnp.bfloat16)
        current = jnp.dot(
            iterate_rows,
            lax.all_gather(shift_low, ROW, axis=0, tiled=True),
            preferred_element_type=jnp.float32,
        )
    summed = over_axes(jnp.stack(partial_list), ROW_COL)
    residual_norms = jnp.sqrt(summed / N)
    return (current, residual_norms)


def solution(mesh):
    split = Mesh(mesh.devices.reshape(4, 4, 4, 2), ("row_0", "row_1", "col_0", "col_1"))
    placed = (P(ROW, COL),)
    return jax.shard_map(
        shards, mesh=split, in_specs=placed, out_specs=(P(ROW, COL), P()), check_vma=False
    )
```

```python
import functools

import jax
import jax.numpy as jnp
from jax import lax
from jax.experimental import pallas as pl
from jax.experimental.pallas import tpu as pltpu
from jax.sharding import PartitionSpec as P

MESH = pl.DeviceIdType.MESH
F32 = jnp.float32
LOW = jnp.bfloat16
A, Y2, Y3 = 0, 1, 2
RA, RT1, RY2, RT2, RY3, RT3 = range(6)
PARTS = 4


def kernel(
    size, mat_hbm, inv_ref, norm_ref, mat_ref, cols, c_cols, rows, c_rows, acc, eye, out_buf, landing, relay,
    part, sum_x, sum_yz,
    col_send, col_recv, row_send, row_recv, sum_send, sum_x_recv, sum_yz_recv,
    out_send, out_recv, relay_send, relay_recv, pass_send, mat_sem,
):
    half = size // 16
    row, col = lax.axis_index("row"), lax.axis_index("col")
    y, z = lax.div(row, 4), lax.rem(row, 4)
    x, c = lax.div(col, 2), lax.rem(col, 2)
    d = 1 - 2 * c

    def ring(v):
        return lax.rem(v + 8, 4)

    def send(src, dst, send_sem, recv_sem, dev_row, dev_col):
        pltpu.make_async_remote_copy(
            src_ref=src, dst_ref=dst, send_sem=send_sem, recv_sem=recv_sem,
            device_id=(dev_row, dev_col), device_id_type=MESH,
        ).start()

    def lines(n):
        return pl.ds(n * (half // PARTS), half // PARTS)

    def wait(ref, sem):
        pltpu.make_async_copy(ref, ref, sem).wait()

    flip_slot = lax.rem(z, 2)
    stays = (x == y) & (c == lax.div(z, 2))

    def flip_self(h):
        return stays & (flip_slot == h)

    barrier = pltpu.get_barrier_semaphore()

    def greet(dev_row, dev_col):
        pl.semaphore_signal(barrier, inc=1, device_id=(dev_row, dev_col), device_id_type=MESH)

    for k in range(1, 8):
        greet(row, lax.rem(col + k, 8))
    for k in range(1, 16):
        greet(lax.rem(row + k, 16), col)
    fetch = pltpu.make_async_copy(mat_hbm, mat_ref, mat_sem)
    fetch.start()

    r0 = lax.broadcasted_iota(jnp.int32, (half, half), 0)
    r1 = lax.broadcasted_iota(jnp.int32, (half, half), 1)
    eye[...] = (r0 == r1).astype(F32)

    def lane_sums(v):
        v = jnp.sum(v.reshape(half // 8, 8, half), axis=0)
        return v[:, : half // 2] + v[:, half // 2 :]

    fetch.wait()
    total = jnp.zeros((8, half // 2), F32)
    for h in range(2):
        block = mat_ref[:, h * half:(h + 1) * half]
        total = total + lane_sums(block * block)
        low = block.astype(LOW)
        cols[A, h * 16 + row] = low
        rows[RA, 2 * col + h] = low
    sum_x[0, col] = total

    pl.semaphore_wait(barrier, 22)

    def at(h, a, b):
        return 4 * a + b if h == 0 else 4 * b + a

    home = ((y, z), (z, y))

    def col_push(g, h, slot_ab, to_ab):
        slot = h * 16 + at(h, *slot_ab)
        send(cols.at[g, slot], cols.at[g, slot], col_send.at[g], col_recv.at[g, slot], at(h, *to_ab), col)

    def col_wait(g, h, slot_ab):
        slot = h * 16 + at(h, *slot_ab)
        wait(cols.at[g, slot], col_recv.at[g, slot])

    def col_start(g):
        for h in range(2):
            a, b = home[h]
            col_push(g, h, (a, b), (ring(a + d), b))
            col_push(g, h, (a, b), (ring(a - d), b))
        for h in range(2):
            a, b = home[h]
            col_push(g, h, (a, b), (a, ring(b + d)))
            col_push(g, h, (a, b), (a, ring(b - d)))

    def col_first(g, k):
        for h in range(2):
            a, b = home[h]
            src = (ring(a + (-d, d, -2 * d)[k]), b)
            col_wait(g, h, src)
            if k == 0:
                col_push(g, h, src, (ring(a + d), b))
            col_push(g, h, src, (a, ring(b + d)))
            col_push(g, h, src, (a, ring(b - d)))

    def col_second(g, k):
        for h in range(2):
            a, b = home[h]
            src = (ring(a + (0, -d, d, -2 * d)[k]), ring(b - d))
            col_wait(g, h, src)
            col_push(g, h, src, (a, ring(b + d)))

    def col_last(g, side):
        for k in range(4):
            for h in range(2):
                a, b = home[h]
                col_wait(g, h, (ring(a + (0, -d, d, -2 * d)[k]), ring(b + (d, -2 * d)[side])))

    def col_drain(g):
        wait(cols.at[g, pl.ds(0, 30)], col_send.at[g])

    def row_slot(px, pc, h):
        return 4 * px + 2 * pc + h

    def row_push(g, slot, px, pc):
        send(rows.at[g, slot], rows.at[g, slot], row_send.at[g], row_recv.at[g, slot], row, 2 * px + pc)

    def row_wait(g, slot):
        wait(rows.at[g, slot], row_recv.at[g, slot])

    def row_open(g, h):
        if h == 0:
            row_push(g, row_slot(x, c, 0), ring(x + 1), c)
        else:
            row_push(g, row_slot(x, c, 1), ring(x - 1), c)
            row_push(g, row_slot(x, c, 1), ring(x + 1), c)
            row_push(g, row_slot(x, c, 0), ring(x - 1), c)
            for k in range(2):
                row_push(g, row_slot(x, c, k), x, 1 - c)

    def row_near(g, first):
        for side, h in ((1, 0 if first else 1), (-1, 1 if first else 0)):
            slot = row_slot(ring(x - side), c, h)
            row_wait(g, slot)
            if first:
                row_push(g, slot, ring(x + side), c)
            row_push(g, slot, x, 1 - c)

    def row_far(g):
        for h in range(2):
            slot = row_slot(ring(x + 2), c, h)
            row_wait(g, slot)
            row_push(g, slot, x, 1 - c)

    def row_mate(g, k):
        for h in range(2):
            row_wait(g, row_slot(ring(x + k), 1 - c, h))

    def row_drain(g):
        wait(rows.at[g, pl.ds(0, 14)], row_send.at[g])

    def summed(buf, count):
        v = buf[0]
        for k in range(1, count):
            v = v + buf[k]
        return v

    def sum_start(t):
        for k in range(1, 8):
            send(sum_x.at[t, col], sum_x.at[t, col], sum_send.at[t, 0], sum_x_recv.at[t, col], row, lax.rem(col + k, 8))

    def sum_mid(t):
        for k in range(1, 8):
            o = lax.rem(col + k, 8)
            wait(sum_x.at[t, o], sum_x_recv.at[t, o])
        sum_yz[t, row] = summed(sum_x.at[t], 8)
        for k in range(1, 16):
            send(sum_yz.at[t, row], sum_yz.at[t, row], sum_send.at[t, 1], sum_yz_recv.at[t, row], lax.rem(row + k, 16), col)

    def sum_done(t):
        for k in range(1, 16):
            o = lax.rem(row + k, 16)
            wait(sum_yz.at[t, o], sum_yz_recv.at[t, o])
        return summed(sum_yz.at[t], 16)

    def sum_drain(t):
        wait(sum_x.at[t, pl.ds(0, 7)], sum_send.at[t, 0])
        wait(sum_yz.at[t, pl.ds(0, 15)], sum_send.at[t, 1])

    def dots(left, right, slots, start=(None, None)):
        total = list(start)
        for h in range(2):
            for q in slots(h) if callable(slots) else slots:
                term = jnp.dot(left[q], right[h * 16 + q], preferred_element_type=F32)
                total[h] = term if total[h] is None else total[h] + term
        return total

    def keep(pieces):
        for h in range(2):
            acc[h] = pieces[h]

    def kept():
        return acc[0], acc[1]

    def by_chip(k):
        return [4 * ring(x + k) + i for i in range(4)]

    def by_plane(*ks):
        def slots(h):
            planes = [ring(home[h][1] + (0, -d, d, -2 * d)[k]) for k in ks]
            return [at(h, i, b) for b in planes for i in range(4)]
        return slots

    def low_start(mat, scale, flag):
        own_eye = eye[...] * flag
        residual = own_eye - mat.astype(F32) * scale
        shift = (own_eye + residual).astype(LOW)
        return residual, (shift.astype(F32) * scale).astype(LOW)

    def is_eye(r, q):
        return (r == q).astype(F32)

    def note_residual(k, h, residual):
        s = jnp.sum(lane_sums(residual * residual), axis=0, keepdims=True)
        if h == 0:
            part[k:k + 1, :] = s
        else:
            part[k:k + 1, :] += s

    def make_shift(k, g, pieces):
        for h in range(2):
            own_eye = eye[...] * is_eye(row, 2 * col + h)
            residual = own_eye - pieces[h]
            rows[g, 2 * col + h] = (own_eye + residual).astype(LOW)
            row_open(g, h)
            note_residual(k, h, residual)

    def make_iterate(g_row, g_col, pieces):
        for h in range(2):
            low = pieces[h].astype(LOW)
            rows[g_row, 2 * col + h] = low
            row_open(g_row, h)
            cols[g_col, h * 16 + row] = low

    sum_start(0)
    for h in range(2):
        row_open(RA, h)
    col_start(A)
    part[...] = jnp.zeros_like(part)
    sum_mid(0)
    col_first(A, 0)
    row_near(RA, True)
    col_first(A, 1)
    row_near(RA, False)
    col_second(A, 0)
    row_far(RA)
    col_first(A, 2)
    col_second(A, 1)
    col_second(A, 2)
    scale = jnp.sqrt(F32(size)) / jnp.sqrt(jnp.full((1, 1), jnp.sum(sum_done(0)), F32))
    scale = scale.astype(LOW).astype(F32)
    for h in range(2):
        residual, _ = low_start(rows[RA, 2 * col + h], scale, is_eye(row, 2 * col + h))
        note_residual(0, h, residual)

    def fill_rows(k):
        def body(i, carry):
            q = 4 * k + i
            c_rows[q] = low_start(rows[RA, q], scale, is_eye(row, q))[1]
            return carry
        lax.fori_loop(0, 4, body, 0)

    for k in range(4):
        row_mate(RA, k)
    for k in range(4):
        fill_rows(k)
    col_second(A, 3)
    keep(dots(c_rows, cols.at[A], by_plane(0, 1)))
    col_last(A, 0)
    keep(dots(c_rows, cols.at[A], by_plane(2), kept()))
    col_last(A, 1)
    make_shift(1, RT1, dots(c_rows, cols.at[A], by_plane(3), kept()))

    def fill_cols(k):
        def body(i, carry):
            r = 4 * k + i
            for h in range(2):
                c_cols[h * 16 + r] = low_start(cols[A, h * 16 + r], scale, is_eye(r, 2 * col + h))[1]
            return carry
        lax.fori_loop(0, 4, body, 0)

    for k in range(4):
        fill_cols(k)
    row_near(RT1, True)
    row_near(RT1, False)
    row_mate(RT1, 0)
    keep(dots(rows.at[RT1], c_cols, by_chip(0)))
    row_far(RT1)
    row_mate(RT1, 1)
    row_mate(RT1, 3)
    keep(dots(rows.at[RT1], c_cols, by_chip(1) + by_chip(3), kept()))
    row_mate(RT1, 2)
    pieces = dots(rows.at[RT1], c_cols, by_chip(2), kept())

    for k, (g_y, g_t, g_c) in ((2, (RY2, RT2, Y2)), (3, (RY3, RT3, Y3))):
        make_iterate(g_y, g_c, pieces)
        col_start(g_c)
        row_near(g_y, True)
        col_first(g_c, 0)
        col_first(g_c, 1)
        row_near(g_y, False)
        col_second(g_c, 0)
        row_mate(g_y, 0)
        keep(dots(rows.at[g_y], cols.at[A], by_chip(0)))
        row_far(g_y)
        row_mate(g_y, 1)
        row_mate(g_y, 3)
        keep(dots(rows.at[g_y], cols.at[A], by_chip(1) + by_chip(3), kept()))
        row_mate(g_y, 2)
        make_shift(k, g_t, dots(rows.at[g_y], cols.at[A], by_chip(2), kept()))
        if k == 3:
            sum_x[1, col] = part[...]
            sum_start(1)
        col_first(g_c, 2)
        col_second(g_c, 1)
        col_second(g_c, 2)
        row_near(g_t, True)
        col_second(g_c, 3)
        row_near(g_t, False)
        row_far(g_t)
        if k == 3:
            sum_mid(1)
        col_last(g_c, 0)
        col_last(g_c, 1)
        row_mate(g_t, 0)
        row_mate(g_t, 1)
        row_mate(g_t, 3)
        keep(dots(rows.at[g_t], cols.at[g_c], by_chip(0) + by_chip(1) + by_chip(3)))
        row_mate(g_t, 2)
        pieces = dots(rows.at[g_t], cols.at[g_c], by_chip(2), kept())

    def flip_out(src, send_sem, h, n, far_x, far_y):
        send(
            src, landing.at[flip_slot, lines(n)], send_sem, out_recv.at[flip_slot, n],
            4 * far_y + 2 * c + h, 2 * far_x + lax.div(z, 2),
        )

    apart = ring(x - y) == 2
    for h in range(2):
        out_buf[h] = pieces[h].T

        @pl.when(apart)
        def _(h=h):
            for n in range(PARTS):
                part_of = out_buf.at[h, lines(n)]
                send(part_of, relay.at[h, lines(n)], out_send.at[h, n], relay_recv.at[h, n], 4 * x + z, col)

        @pl.when(jnp.logical_not(apart | flip_self(h)))
        def _(h=h):
            for n in range(PARTS):
                flip_out(out_buf.at[h, lines(n)], out_send.at[h, n], h, n, y, x)

        @pl.when(flip_self(h))
        def _(h=h):
            landing[h] = out_buf[h]

    @pl.when(x == y)
    def _():
        for h in range(2):
            for n in range(PARTS):
                wait(relay.at[h, lines(n)], relay_recv.at[h, n])
                flip_out(relay.at[h, lines(n)], pass_send.at[h, n], h, n, ring(x + 2), x)

    norms = jnp.sqrt(jnp.sum(sum_done(1), axis=1, keepdims=True) / F32(size))
    for k in range(4):
        norm_ref[k] = norms[k, 0]
    for g in range(3):
        col_drain(g)
    for g in range(6):
        row_drain(g)
    for t in range(2):
        sum_drain(t)
    @pl.when(x == y)
    def _():
        for h in range(2):
            for n in range(PARTS):
                wait(relay.at[h, lines(n)], pass_send.at[h, n])

    for h in range(2):
        @pl.when(jnp.logical_not(flip_self(h)))
        def _(h=h):
            for n in range(PARTS):
                wait(out_buf.at[h, lines(n)], out_send.at[h, n])
                wait(landing.at[h, lines(n)], out_recv.at[h, n])
        inv_ref[:, h * half:(h + 1) * half] = landing[h]


def solution(mesh):
    def shards(matrix):
        b = matrix.shape[0]
        return pl.pallas_call(
            functools.partial(kernel, 16 * b),
            out_shape=(
                jax.ShapeDtypeStruct((b, 2 * b), F32),
                jax.ShapeDtypeStruct((4,), F32),
            ),
            in_specs=[pl.BlockSpec(memory_space=pltpu.HBM)],
            out_specs=(
                pl.BlockSpec(memory_space=pltpu.VMEM),
                pl.BlockSpec(memory_space=pltpu.SMEM),
            ),
            scratch_shapes=[
                pltpu.VMEM((b, 2 * b), F32),
                pltpu.VMEM((3, 32, b, b), LOW),
                pltpu.VMEM((32, b, b), LOW),
                pltpu.VMEM((6, 16, b, b), LOW),
                pltpu.VMEM((16, b, b), LOW),
                pltpu.VMEM((2, b, b), F32),
                pltpu.VMEM((b, b), F32),
                pltpu.VMEM((2, b, b), F32),
                pltpu.VMEM((2, b, b), F32),
                pltpu.VMEM((2, b, b), F32),
                pltpu.VMEM((8, b // 2), F32),
                pltpu.VMEM((2, 8, 8, b // 2), F32),
                pltpu.VMEM((2, 16, 8, b // 2), F32),
                pltpu.SemaphoreType.DMA((3,)),
                pltpu.SemaphoreType.DMA((3, 32)),
                pltpu.SemaphoreType.DMA((6,)),
                pltpu.SemaphoreType.DMA((6, 16)),
                pltpu.SemaphoreType.DMA((2, 2)),
                pltpu.SemaphoreType.DMA((2, 8)),
                pltpu.SemaphoreType.DMA((2, 16)),
                pltpu.SemaphoreType.DMA((2, PARTS)),
                pltpu.SemaphoreType.DMA((2, PARTS)),
                pltpu.SemaphoreType.DMA((2, PARTS)),
                pltpu.SemaphoreType.DMA((2, PARTS)),
                pltpu.SemaphoreType.DMA((2, PARTS)),
                pltpu.SemaphoreType.DMA,
            ],
            compiler_params=pltpu.CompilerParams(collective_id=0, has_side_effects=True, vmem_limit_bytes=40 * 1024 * 1024),
        )(matrix)

    return jax.shard_map(
        shards, mesh=mesh, in_specs=(P("row", "col"),), out_specs=(P("row", "col"), P()), check_vma=False
    )
```
